32 devices in a mesh: pb: 4 (over y, x), neg: 8 (over z, core).
Axes of the slice: x: 2, y: 2, z: 4, core: 2. Of those that a mesh axis runs over, the one named last changes fastest.
Arguments:
- hidden: bfloat16 [4, 32, 128, 1024], P('pb', 'neg'), may hold values from -6 to 6
- lengths: int32 [4, 32], P('pb', 'neg'), may hold values from 32 to 128
- teacher: float32 [4, 32], P('pb', 'neg'), may hold values from -8 to 8
- norm_gain: float32 [1024], replicated, may hold values from 0.1 to 1.9
- final_gain: float32 [1024], replicated, may hold values from 0.1 to 1.9
- score_vector: float32 [1024], replicated, may hold values from -0.1875 to 0.1875
- query_weight: bfloat16 [1024, 1024], P(('pb', 'neg')), may hold values from -0.1875 to 0.1875
- key_matrix: bfloat16 [1024, 512], P(('pb', 'neg')), may hold values from -0.1875 to 0.1875
- value_matrix: bfloat16 [1024, 512], P(('pb', 'neg')), may hold values from -0.1875 to 0.1875
- out_weight: bfloat16 [1024, 1024], P(None, ('pb', 'neg')), may hold values from -0.1875 to 0.1875
Outputs:
- scores: float32 [4, 32], P('pb', 'neg')
- loss: float32 [], replicated
- grad_hidden: bfloat16 [4, 32, 128, 1024], P('pb', 'neg')
- grad_query: float32 [1024, 1024], P(('pb', 'neg'))
- grad_key: float32 [1024, 512], P(('pb', 'neg'))
- grad_value: float32 [1024, 512], P(('pb', 'neg'))
- grad_out: float32 [1024, 1024], P(None, ('pb', 'neg'))
The draws below stay inside these ranges and needn't reach their ends.
Inputs may be any that keep to these rules, and one draw needn't show every extreme that they name: `lengths`: the number of real tokens of the pair; its other positions out of 128 are padding.
All inputs are finite; a program needn't handle non-finite values.
Results may differ from the reference program's by a relative error of at most 0.013.
Values may be sent and summed in bfloat16 or wider, within the bound.
A program may use at most 64 MiB of HBM per device.

```python
import jax
import jax.numpy as jnp
from jax import lax

HIDDEN_WIDTH = 1024
HQ = 8
KEY_VALUE_HEADS = 4
HEAD_WIDTH = 128
SEQ = 128
PAIR_DEV = 4
QUERIES = 4
LIST = 32


def place_ends(array, key, smallest, largest):
    shape = array.shape
    index_at = [jax.random.randint(jax.random.fold_in(key, axis), (), 0, shape[axis]) for axis in range(len(shape))]
    array = array.at[tuple(index_at)].set(smallest)
    longest = shape.index(max(shape))
    index_at[longest] = (index_at[longest] + 1) % shape[longest]
    return array.at[tuple(index_at)].set(largest)


def levels(own_key, extent, cuts, least, high):
    loudness = 1.0
    for position, shards_of in cuts:
        heights = jax.random.uniform(jax.random.fold_in(jax.random.fold_in(own_key, 6), position), (shards_of,), jnp.float32, least / len(cuts), high / len(cuts))
        loudness = loudness * jnp.repeat(jnp.exp(heights), extent[position] // shards_of).reshape((-1,) + (1,) * (len(extent) - 1 - position))
    return loudness


def bell_draw(rng, dims, scale, bound, split=(), kind=jnp.bfloat16):
    array = jax.random.normal(rng, dims, jnp.float32) * scale
    if len(split) > 0:
        array = levels(rng, dims, split, -0.22, 0.18) * array
    return jnp.clip(array, min=-bound, max=bound).astype(kind)


def setup_inputs(seed: int = 0) -> dict:
    keys = jax.random.split(jax.random.key(seed), 11)
    hidden = bell_draw(keys[0], (QUERIES, LIST, SEQ, HIDDEN_WIDTH), 1.0, 6.0, ((0, 4), (1, 8)))
    lengths = place_ends(jax.random.randint(keys[1], (QUERIES, LIST), SEQ // 4, SEQ + 1), jax.random.fold_in(keys[1], 1), SEQ // 4, SEQ).astype(jnp.int32)
    teacher = bell_draw(keys[2], (QUERIES, LIST), 2.0, 8.0, ((0, 4), (1, 8)), jnp.float32)
    norm_gain = jnp.clip(1.0 + 0.18 * jax.random.normal(keys[3], (HIDDEN_WIDTH,), jnp.float32), 0.1, 1.9)
    final_gain = jnp.clip(1.0 + 0.18 * jax.random.normal(keys[4], (HIDDEN_WIDTH,), jnp.float32), 0.1, 1.9)
    score_vector = bell_draw(keys[5], (HIDDEN_WIDTH,), HIDDEN_WIDTH ** -0.5, 0.1875, (), jnp.float32)
    query_weight = bell_draw(keys[6], (HIDDEN_WIDTH, HQ * HEAD_WIDTH), HIDDEN_WIDTH ** -0.5, 0.1875, ((0, 32),))
    key_matrix = bell_draw(keys[7], (HIDDEN_WIDTH, KEY_VALUE_HEADS * HEAD_WIDTH), HIDDEN_WIDTH ** -0.5, 0.1875, ((0, 32),))
    value_matrix = bell_draw(keys[8], (HIDDEN_WIDTH, KEY_VALUE_HEADS * HEAD_WIDTH), HIDDEN_WIDTH ** -0.5, 0.1875, ((0, 32),))
    out_weight = bell_draw(keys[9], (HQ * HEAD_WIDTH, HIDDEN_WIDTH), (HQ * HEAD_WIDTH) ** -0.5, 0.1875, ((1, 32),))
    return dict(hidden=hidden, lengths=lengths, teacher=teacher, norm_gain=norm_gain, final_gain=final_gain, score_vector=score_vector, query_weight=query_weight, key_matrix=key_matrix, value_matrix=value_matrix, out_weight=out_weight)


EPSILON = 1e-06
ROPE_BASE = 1000000.0
TEACHER_TEMP = 2.0
GRAD_SCALE = 512.0

def rope_tables(seq_len, head_size):
    half = head_size // 2
    freqs = ROPE_BASE ** (-(jnp.arange(half, dtype=jnp.float32) * 2.0) / head_size)
    angles = jnp.arange(seq_len, dtype=jnp.float32)[:, None] * freqs[None, :]
    angles = jnp.concatenate([angles, angles], axis=1)
    return (jnp.cos(angles), jnp.sin(angles))

def rotate_half(vector):
    half = vector.shape[-1] // 2
    return jnp.concatenate([-vector[..., half:], vector[..., :half]], axis=-1)

def unrotate_half(vector):
    half = vector.shape[-1] // 2
    return jnp.concatenate([vector[..., half:], -vector[..., :half]], axis=-1)

def forward_pairs(tokens_in, lengths_here, norm_gain, final_gain, score_vector, query_weight, key_matrix, value_matrix, out_weight):
    pair_count, seq_len, model_width = tokens_in.shape
    head_count = query_weight.shape[1] // HEAD_WIDTH
    group_count = key_matrix.shape[1] // HEAD_WIDTH
    group_size = head_count // group_count
    inputs_wide = tokens_in.astype(jnp.float32)
    inv_rms = lax.rsqrt(lax.optimization_barrier(jnp.mean(inputs_wide * inputs_wide, axis=-1, keepdims=True)) + EPSILON)
    normed = (inputs_wide * inv_rms * norm_gain).astype(jnp.bfloat16)
    flat_rows = normed.reshape(pair_count * seq_len, model_width)
    key_proj = jnp.dot(flat_rows, key_matrix, preferred_element_type=jnp.float32).reshape(pair_count, seq_len, group_count, HEAD_WIDTH)
    value_proj = jnp.dot(flat_rows, value_matrix, preferred_element_type=jnp.float32).reshape(pair_count, seq_len, group_count, HEAD_WIDTH)
    positions = jnp.arange(seq_len, dtype=jnp.int32)
    last_index = (lengths_here - 1).astype(jnp.int32)
    onehot = (positions[None, :] == last_index[:, None]).astype(jnp.float32)
    normed_last = jnp.take_along_axis(normed, last_index[:, None, None], axis=1)[:, 0]
    query_proj = jnp.dot(normed_last, query_weight, preferred_element_type=jnp.float32).reshape(pair_count, head_count, HEAD_WIDTH)
    query_scale = lax.rsqrt(lax.optimization_barrier(jnp.mean(query_proj * query_proj, axis=-1, keepdims=True)) + EPSILON)
    query_unit = query_proj * query_scale
    key_scale = lax.rsqrt(lax.optimization_barrier(jnp.mean(key_proj * key_proj, axis=-1, keepdims=True)) + EPSILON)
    key_unit = key_proj * key_scale
    cos_table, sin_table = rope_tables(seq_len, HEAD_WIDTH)
    cos_query = jnp.dot(onehot, cos_table, precision=lax.Precision.HIGHEST)
    sin_query = jnp.dot(onehot, sin_table, precision=lax.Precision.HIGHEST)
    query_rot = (query_unit * cos_query[:, None, :] + rotate_half(query_unit) * sin_query[:, None, :]).astype(jnp.bfloat16)
    key_rot = (key_unit * cos_table[None, :, None, :] + rotate_half(key_unit) * sin_table[None, :, None, :]).astype(jnp.bfloat16)
    value_cast = value_proj.astype(jnp.bfloat16)
    grouped = query_rot.reshape(pair_count, group_count, group_size, HEAD_WIDTH)
    logits = jnp.einsum('pkgd,pskd->pkgs', grouped.astype(jnp.float32), key_rot.astype(jnp.float32)) * HEAD_WIDTH ** (-0.5)
    visible = (positions[None, :] <= last_index[:, None])[:, None, None, :]
    expos = jnp.where(visible, jnp.exp(logits), 0.0)
    attention_weights = expos / lax.optimization_barrier(jnp.sum(expos, axis=-1, keepdims=True))
    probs_cast = attention_weights.astype(jnp.bfloat16)
    context = jnp.einsum('pkgs,pskd->pkgd', probs_cast.astype(jnp.float32), value_cast.astype(jnp.float32))
    context = context.astype(jnp.bfloat16).reshape(pair_count, head_count * HEAD_WIDTH)
    attended = jnp.dot(context, out_weight, preferred_element_type=jnp.float32)
    residual = jnp.take_along_axis(inputs_wide, last_index[:, None, None], axis=1)[:, 0] + attended
    out_scale = lax.rsqrt(lax.optimization_barrier(jnp.mean(residual * residual, axis=-1, keepdims=True)) + EPSILON)
    out_unit = residual * out_scale
    scores_here = lax.optimization_barrier(jnp.sum(out_unit * final_gain * score_vector, axis=-1))
    stored = (tokens_in, onehot, inv_rms, normed, normed_last, query_unit, query_scale, key_unit, key_scale, cos_query, sin_query, cos_table, sin_table, query_rot, key_rot, value_cast, attention_weights, probs_cast, context, out_unit, out_scale)
    return (scores_here, stored)

def backward_pairs(stored, grad_score, norm_gain, final_gain, score_vector, query_weight, key_matrix, value_matrix, out_weight):
    tokens_in, onehot, inv_rms, normed, normed_last, query_unit, query_scale, key_unit, key_scale, cos_query, sin_query, cos_table, sin_table, query_rot, key_rot, value_cast, attention_weights, probs_cast, context, out_unit, out_scale = stored
    pair_count, seq_len, model_width = tokens_in.shape
    head_count = query_weight.shape[1] // HEAD_WIDTH
    group_count = key_matrix.shape[1] // HEAD_WIDTH
    group_size = head_count // group_count
    grad_unit = grad_score[:, None] * score_vector * final_gain
    grad_resid = out_scale * (grad_unit - out_unit * lax.optimization_barrier(jnp.mean(grad_unit * out_unit, axis=-1, keepdims=True)))
    grad_resid_cast = grad_resid.astype(jnp.bfloat16)
    grad_out = jnp.dot(context.T, grad_resid_cast, preferred_element_type=jnp.float32)
    grad_context = jnp.dot(grad_resid_cast, out_weight.T, preferred_element_type=jnp.float32).astype(jnp.bfloat16)
    grad_context = grad_context.reshape(pair_count, group_count, group_size, HEAD_WIDTH).astype(jnp.float32)
    grad_probs = jnp.einsum('pkgd,pskd->pkgs', grad_context, value_cast.astype(jnp.float32))
    grad_vals = jnp.einsum('pkgs,pkgd->pskd', probs_cast.astype(jnp.float32), grad_context)
    spread = lax.optimization_barrier(jnp.sum(attention_weights * grad_probs, axis=-1, keepdims=True))
    logit_gradient = (attention_weights * (grad_probs - spread)).astype(jnp.bfloat16).astype(jnp.float32)
    grouped = query_rot.reshape(pair_count, group_count, group_size, HEAD_WIDTH).astype(jnp.float32)
    rotated_query_gradient = jnp.einsum('pkgs,pskd->pkgd', logit_gradient, key_rot.astype(jnp.float32)) * HEAD_WIDTH ** (-0.5)
    rotated_query_gradient = rotated_query_gradient.reshape(pair_count, head_count, HEAD_WIDTH)
    grad_krot = jnp.einsum('pkgs,pkgd->pskd', logit_gradient, grouped) * HEAD_WIDTH ** (-0.5)
    grad_qunit = rotated_query_gradient * cos_query[:, None, :] + unrotate_half(rotated_query_gradient * sin_query[:, None, :])
    grad_kunit = grad_krot * cos_table[None, :, None, :] + unrotate_half(grad_krot * sin_table[None, :, None, :])
    grad_qproj = query_scale * (grad_qunit - query_unit * lax.optimization_barrier(jnp.mean(grad_qunit * query_unit, axis=-1, keepdims=True)))
    grad_kproj = key_scale * (grad_kunit - key_unit * lax.optimization_barrier(jnp.mean(grad_kunit * key_unit, axis=-1, keepdims=True)))
    grad_q_cast = grad_qproj.reshape(pair_count, head_count * HEAD_WIDTH).astype(jnp.bfloat16)
    grad_k_cast = grad_kproj.reshape(pair_count * seq_len, group_count * HEAD_WIDTH).astype(jnp.bfloat16)
    grad_v_cast = grad_vals.reshape(pair_count * seq_len, group_count * HEAD_WIDTH).astype(jnp.bfloat16)
    flat_rows = normed.reshape(pair_count * seq_len, model_width)
    grad_query = jnp.dot(normed_last.T, grad_q_cast, preferred_element_type=jnp.float32)
    grad_key = jnp.dot(flat_rows.T, grad_k_cast, preferred_element_type=jnp.float32)
    grad_value = jnp.dot(flat_rows.T, grad_v_cast, preferred_element_type=jnp.float32)
    grad_normed = jnp.dot(grad_k_cast, key_matrix.T, preferred_element_type=jnp.float32)
    grad_normed = grad_normed + jnp.dot(grad_v_cast, value_matrix.T, preferred_element_type=jnp.float32)
    grad_normed = grad_normed.reshape(pair_count, seq_len, model_width)
    grad_last = jnp.dot(grad_q_cast, query_weight.T, preferred_element_type=jnp.float32)
    grad_normed = grad_normed + onehot[:, :, None] * grad_last[:, None, :]
    inputs_wide = tokens_in.astype(jnp.float32)
    grad_scaled = grad_normed * norm_gain
    grad_input = inv_rms * grad_scaled - inputs_wide * inv_rms * inv_rms * inv_rms * lax.optimization_barrier(jnp.mean(grad_scaled * inputs_wide, axis=-1, keepdims=True))
    grad_input = grad_input + onehot[:, :, None] * grad_resid[:, None, :]
    return (grad_input.astype(jnp.bfloat16), (grad_query, grad_key, grad_value, grad_out))

def reference(hidden, lengths, teacher, norm_gain, final_gain, score_vector, query_weight, key_matrix, value_matrix, out_weight):
    query_count, list_len, seq_len, model_width = hidden.shape
    block_count = list_len // PAIR_DEV
    weights = (query_weight, key_matrix, value_matrix, out_weight)

    def score_block(carry, item):
        block_tokens, block_lengths = item
        block_scores, stored = forward_pairs(block_tokens, block_lengths, norm_gain, final_gain, score_vector, weights[0], weights[1], weights[2], weights[3])
        return (carry, block_scores)
    score_rows = []
    for query_pos in range(query_count):
        blocks_in = hidden[query_pos].reshape(block_count, PAIR_DEV, seq_len, model_width)
        blocks_len = lengths[query_pos].reshape(block_count, PAIR_DEV)
        carry_out, block_scores = lax.scan(score_block, jnp.zeros((), jnp.float32), (blocks_in, blocks_len))
        score_rows.append(block_scores.reshape(list_len))
    scores = jnp.stack(score_rows, axis=0)
    scaled = teacher / TEACHER_TEMP
    expo_s = jnp.exp(scores)
    expo_t = jnp.exp(scaled)
    total_s = lax.optimization_barrier(jnp.sum(expo_s, axis=-1, keepdims=True))
    total_t = lax.optimization_barrier(jnp.sum(expo_t, axis=-1, keepdims=True))
    prob_s = expo_s / total_s
    prob_t = expo_t / total_t
    loss = jnp.sum(prob_t * (scaled - jnp.log(total_t) - (scores - jnp.log(total_s))))
    grad_score = GRAD_SCALE * (prob_s - prob_t)

    def grad_block(carry, item):
        block_tokens, block_lengths, block_grad = item
        block_scores, stored = forward_pairs(block_tokens, block_lengths, norm_gain, final_gain, score_vector, weights[0], weights[1], weights[2], weights[3])
        grad_input, grads = backward_pairs(stored, block_grad, norm_gain, final_gain, score_vector, weights[0], weights[1], weights[2], weights[3])
        summed = (carry[0] + grads[0], carry[1] + grads[1], carry[2] + grads[2], carry[3] + grads[3])
        return (summed, grad_input)
    total_blocks = query_count * block_count
    start = (jnp.zeros(query_weight.shape, jnp.float32), jnp.zeros(key_matrix.shape, jnp.float32), jnp.zeros(value_matrix.shape, jnp.float32), jnp.zeros(out_weight.shape, jnp.float32))
    items = (hidden.reshape(total_blocks, PAIR_DEV, seq_len, model_width), lengths.reshape(total_blocks, PAIR_DEV), grad_score.reshape(total_blocks, PAIR_DEV))
    grads, grad_blocks = lax.scan(grad_block, start, items)
    grad_hidden = grad_blocks.reshape(query_count, list_len, seq_len, model_width)
    return (scores, loss, grad_hidden, grads[0], grads[1], grads[2], grads[3])
```

```python
import jax
import jax.numpy as jnp
from jax import lax
from jax.sharding import PartitionSpec as P

HEAD_WIDTH = 128


EPSILON = 1e-06
ROPE_BASE = 1000000.0
TEACHER_TEMP = 2.0
GRAD_SCALE = 512.0


def rope_tables(seq_len, head_size):
    half = head_size // 2
    freqs = ROPE_BASE ** (-(jnp.arange(half, dtype=jnp.float32) * 2.0) / head_size)
    angles = jnp.arange(seq_len, dtype=jnp.float32)[:, None] * freqs[None, :]
    angles = jnp.concatenate([angles, angles], axis=1)
    return (jnp.cos(angles), jnp.sin(angles))


def rotate_half(vector):
    half = vector.shape[-1] // 2
    return jnp.concatenate([-vector[..., half:], vector[..., :half]], axis=-1)


def unrotate_half(vector):
    half = vector.shape[-1] // 2
    return jnp.concatenate([vector[..., half:], -vector[..., :half]], axis=-1)


def forward_pairs(
    tokens_in,
    lengths_here,
    norm_gain,
    final_gain,
    score_vector,
    query_weight,
    key_matrix,
    value_matrix,
    out_weight,
):
    pair_count, seq_len, model_width = tokens_in.shape
    head_count = query_weight.shape[1] // HEAD_WIDTH
    group_count = key_matrix.shape[1] // HEAD_WIDTH
    group_size = head_count // group_count
    inputs_wide = tokens_in.astype(jnp.float32)
    inv_rms = lax.rsqrt(jnp.mean(inputs_wide * inputs_wide, axis=-1, keepdims=True) + EPSILON)
    normed = (inputs_wide * inv_rms * norm_gain).astype(jnp.bfloat16)
    flat_rows = normed.reshape(pair_count * seq_len, model_width)
    key_proj = jnp.dot(flat_rows, key_matrix, preferred_element_type=jnp.float32).reshape(
        pair_count, seq_len, group_count, HEAD_WIDTH
    )
    value_proj = jnp.dot(flat_rows, value_matrix, preferred_element_type=jnp.float32).reshape(
        pair_count, seq_len, group_count, HEAD_WIDTH
    )
    positions = jnp.arange(seq_len, dtype=jnp.int32)
    last_index = lengths_here - 1
    onehot = (positions[None, :] == last_index[:, None]).astype(jnp.float32)
    normed_last = jnp.take_along_axis(normed, last_index[:, None, None], axis=1)[:, 0]
    query_proj = jnp.dot(normed_last, query_weight, preferred_element_type=jnp.float32).reshape(
        pair_count, head_count, HEAD_WIDTH
    )
    query_scale = lax.rsqrt(jnp.mean(query_proj * query_proj, axis=-1, keepdims=True) + EPSILON)
    query_unit = query_proj * query_scale
    key_scale = lax.rsqrt(jnp.mean(key_proj * key_proj, axis=-1, keepdims=True) + EPSILON)
    key_unit = key_proj * key_scale
    cos_table, sin_table = rope_tables(seq_len, HEAD_WIDTH)
    cos_query = jnp.dot(onehot, cos_table, precision=lax.Precision.HIGHEST)
    sin_query = jnp.dot(onehot, sin_table, precision=lax.Precision.HIGHEST)
    query_rot = (
        query_unit * cos_query[:, None, :] + rotate_half(query_unit) * sin_query[:, None, :]
    ).astype(jnp.bfloat16)
    key_rot = (
        key_unit * cos_table[None, :, None, :] + rotate_half(key_unit) * sin_table[None, :, None, :]
    ).astype(jnp.bfloat16)
    value_cast = value_proj.astype(jnp.bfloat16)
    grouped = query_rot.reshape(pair_count, group_count, group_size, HEAD_WIDTH)
    logits = jnp.einsum(
        "pkgd,pskd->pkgs", grouped, key_rot, preferred_element_type=jnp.float32
    ) * HEAD_WIDTH ** (-0.5)
    visible = (positions[None, :] <= last_index[:, None])[:, None, None, :]
    expos = jnp.where(visible, jnp.exp(logits), 0.0)
    attention_weights = expos / jnp.sum(expos, axis=-1, keepdims=True)
    probs_cast = attention_weights.astype(jnp.bfloat16)
    context = jnp.einsum(
        "pkgs,pskd->pkgd", probs_cast, value_cast, preferred_element_type=jnp.float32
    )
    context = context.astype(jnp.bfloat16).reshape(pair_count, head_count * HEAD_WIDTH)
    attended = jnp.dot(context, out_weight, preferred_element_type=jnp.float32)
    residual = jnp.take_along_axis(inputs_wide, last_index[:, None, None], axis=1)[:, 0] + attended
    out_scale = lax.rsqrt(jnp.mean(residual * residual, axis=-1, keepdims=True) + EPSILON)
    out_unit = residual * out_scale
    scores_here = jnp.sum(out_unit * final_gain * score_vector, axis=-1)
    stored = (
        tokens_in,
        onehot,
        inv_rms,
        normed,
        normed_last,
        query_unit,
        query_scale,
        key_unit,
        key_scale,
        cos_query,
        sin_query,
        cos_table,
        sin_table,
        query_rot,
        key_rot,
        value_cast,
        attention_weights,
        probs_cast,
        context,
        out_unit,
        out_scale,
    )
    return (scores_here, stored)


def backward_pairs(
    stored,
    grad_score,
    norm_gain,
    final_gain,
    score_vector,
    query_weight,
    key_matrix,
    value_matrix,
    out_weight,
):
    (
        tokens_in,
        onehot,
        inv_rms,
        normed,
        normed_last,
        query_unit,
        query_scale,
        key_unit,
        key_scale,
        cos_query,
        sin_query,
        cos_table,
        sin_table,
        query_rot,
        key_rot,
        value_cast,
        attention_weights,
        probs_cast,
        context,
        out_unit,
        out_scale,
    ) = stored
    pair_count, seq_len, model_width = tokens_in.shape
    head_count = query_weight.shape[1] // HEAD_WIDTH
    group_count = key_matrix.shape[1] // HEAD_WIDTH
    group_size = head_count // group_count
    grad_unit = grad_score[:, None] * score_vector * final_gain
    grad_resid = out_scale * (
        grad_unit - out_unit * jnp.mean(grad_unit * out_unit, axis=-1, keepdims=True)
    )
    grad_resid_cast = grad_resid.astype(jnp.bfloat16)
    grad_context = jnp.dot(
        grad_resid_cast, out_weight.T, preferred_element_type=jnp.float32
    ).astype(jnp.bfloat16)
    grad_context = grad_context.reshape(pair_count, group_count, group_size, HEAD_WIDTH)
    grad_probs = jnp.einsum(
        "pkgd,pskd->pkgs", grad_context, value_cast, preferred_element_type=jnp.float32
    )
    grad_vals = jnp.einsum(
        "pkgs,pkgd->pskd", probs_cast, grad_context, preferred_element_type=jnp.float32
    )
    spread = jnp.sum(attention_weights * grad_probs, axis=-1, keepdims=True)
    logit_gradient = (attention_weights * (grad_probs - spread)).astype(jnp.bfloat16)
    grouped = query_rot.reshape(pair_count, group_count, group_size, HEAD_WIDTH)
    rotated_query_gradient = jnp.einsum(
        "pkgs,pskd->pkgd", logit_gradient, key_rot, preferred_element_type=jnp.float32
    ) * HEAD_WIDTH ** (-0.5)
    rotated_query_gradient = rotated_query_gradient.reshape(pair_count, head_count, HEAD_WIDTH)
    grad_krot = jnp.einsum(
        "pkgs,pkgd->pskd", logit_gradient, grouped, preferred_element_type=jnp.float32
    ) * HEAD_WIDTH ** (-0.5)
    grad_qunit = rotated_query_gradient * cos_query[:, None, :] + unrotate_half(
        rotated_query_gradient * sin_query[:, None, :]
    )
    grad_kunit = grad_krot * cos_table[None, :, None, :] + unrotate_half(
        grad_krot * sin_table[None, :, None, :]
    )
    grad_qproj = query_scale * (
        grad_qunit - query_unit * jnp.mean(grad_qunit * query_unit, axis=-1, keepdims=True)
    )
    grad_kproj = key_scale * (
        grad_kunit - key_unit * jnp.mean(grad_kunit * key_unit, axis=-1, keepdims=True)
    )
    grad_q_cast = grad_qproj.reshape(pair_count, head_count * HEAD_WIDTH).astype(jnp.bfloat16)
    grad_k_cast = grad_kproj.reshape(pair_count * seq_len, group_count * HEAD_WIDTH).astype(
        jnp.bfloat16
    )
    grad_v_cast = grad_vals.reshape(pair_count * seq_len, group_count * HEAD_WIDTH).astype(
        jnp.bfloat16
    )
    flat_rows = normed.reshape(pair_count * seq_len, model_width)
    last_rows = jnp.concatenate([normed_last, grad_resid_cast, grad_q_cast, context], axis=1)
    grad_kv = jnp.dot(
        flat_rows.T,
        jnp.concatenate([grad_k_cast, grad_v_cast], axis=1),
        preferred_element_type=jnp.float32,
    )
    grad_normed = jnp.dot(grad_k_cast, key_matrix.T, preferred_element_type=jnp.float32)
    grad_normed = grad_normed + jnp.dot(
        grad_v_cast, value_matrix.T, preferred_element_type=jnp.float32
    )
    grad_normed = grad_normed.reshape(pair_count, seq_len, model_width)
    grad_last = jnp.dot(grad_q_cast, query_weight.T, preferred_element_type=jnp.float32)
    grad_normed = grad_normed + onehot[:, :, None] * grad_last[:, None, :]
    inputs_wide = tokens_in.astype(jnp.float32)
    grad_scaled = grad_normed * norm_gain
    grad_input = inv_rms * grad_scaled - inputs_wide * inv_rms * inv_rms * inv_rms * jnp.mean(
        grad_scaled * inputs_wide, axis=-1, keepdims=True
    )
    grad_input = grad_input + onehot[:, :, None] * grad_resid[:, None, :]
    return (grad_input.astype(jnp.bfloat16), last_rows, grad_kv)


def shards(
    hidden,
    lengths,
    teacher,
    norm_gain,
    final_gain,
    score_vector,
    query_weight,
    key_matrix,
    value_matrix,
    out_weight,
):
    both = ("pb", "neg")
    width = query_weight.shape[1]
    kv_width = key_matrix.shape[1]
    head_width = out_weight.shape[0]
    packed = jnp.concatenate([query_weight, key_matrix, value_matrix, out_weight.T], axis=1)
    everything = lax.all_gather(packed, both, axis=0, tiled=True)
    full_query = everything[:, :width]
    full_key = everything[:, width : width + kv_width]
    full_value = everything[:, width + kv_width : width + 2 * kv_width]
    full_out_t = everything[:, width + 2 * kv_width :]
    scores_here, stored = forward_pairs(
        hidden[0],
        lengths[0],
        norm_gain,
        final_gain,
        score_vector,
        full_query,
        full_key,
        full_value,
        full_out_t.T,
    )
    pair_count = scores_here.shape[0]
    row = lax.axis_index("pb")
    listed = lax.all_gather(jnp.concatenate([scores_here, teacher[0]])[None], both, axis=0, tiled=True)
    listed = listed.reshape(lax.axis_size("pb"), -1, 2, pair_count)
    all_scores = listed[:, :, 0].reshape(listed.shape[0], -1)
    all_scaled = listed[:, :, 1].reshape(listed.shape[0], -1) / TEACHER_TEMP
    total_s = jnp.sum(jnp.exp(all_scores), axis=1, keepdims=True)
    expo_t = jnp.exp(all_scaled)
    total_t = jnp.sum(expo_t, axis=1, keepdims=True)
    loss_value = jnp.sum(
        expo_t
        / total_t
        * (all_scaled - jnp.log(total_t) - (all_scores - jnp.log(total_s)))
    )
    mine = (jnp.arange(listed.shape[0]) == row)[:, None]
    my_total_s = jnp.sum(jnp.where(mine, total_s, 0.0))
    my_total_t = jnp.sum(jnp.where(mine, total_t, 0.0))
    prob_s = jnp.exp(scores_here) / my_total_s
    prob_t = jnp.exp(teacher[0] / TEACHER_TEMP) / my_total_t
    grad_score = GRAD_SCALE * (prob_s - prob_t)
    grad_input, last_rows, grad_kv = backward_pairs(
        stored,
        grad_score,
        norm_gain,
        final_gain,
        score_vector,
        full_query,
        full_key,
        full_value,
        full_out_t.T,
    )
    reduced = lax.psum_scatter(grad_kv.astype(jnp.bfloat16), both, scatter_dimension=0, tiled=True)
    reduced = reduced.astype(jnp.float32)
    rows = lax.all_gather(last_rows, both, axis=0, tiled=True)
    index = row * lax.axis_size("neg") + lax.axis_index("neg")
    share = query_weight.shape[0]
    model_width = share * lax.axis_size("pb") * lax.axis_size("neg")
    out_share = out_weight.shape[1]
    normed_cols = lax.dynamic_slice_in_dim(rows, index * share, share, axis=1)
    resid_cols = lax.dynamic_slice_in_dim(rows, model_width + index * out_share, out_share, axis=1)
    rest = 2 * model_width
    all_q = rows[:, rest : rest + width]
    all_context = rows[:, rest + width :]
    grad_query = jnp.dot(normed_cols.T, all_q, preferred_element_type=jnp.float32)
    grad_out = jnp.dot(all_context.T, resid_cols, preferred_element_type=jnp.float32)
    return (
        scores_here[None],
        loss_value,
        grad_input[None],
        grad_query,
        reduced[:, :kv_width],
        reduced[:, kv_width:],
        grad_out,
    )


def solution(mesh):
    placed = (
        P("pb", "neg", None, None),
        P("pb", "neg"),
        P("pb", "neg"),
        P(),
        P(),
        P(),
        P(("pb", "neg"), None),
        P(("pb", "neg"), None),
        P(("pb", "neg"), None),
        P(None, ("pb", "neg")),
    )
    return jax.shard_map(
        shards,
        mesh=mesh,
        in_specs=placed,
        out_specs=(
            P("pb", "neg"),
            P(),
            P("pb", "neg", None, None),
            P(("pb", "neg"), None),
            P(("pb", "neg"), None),
            P(("pb", "neg"), None),
            P(None, ("pb", "neg")),
        ),
        check_vma=False,
    )
```

```python
import jax
import jax.numpy as jnp
from jax import lax
from jax.experimental import pallas as pl
from jax.experimental.pallas import tpu as pltpu
from jax.sharding import PartitionSpec as P

HEAD_WIDTH = 128
MESH_ID = pl.DeviceIdType.MESH

EPSILON = 1e-06
ROPE_BASE = 1000000.0
TEACHER_TEMP = 2.0
GRAD_SCALE = 512.0


def rope_tables(seq_len, head_size):
    half = head_size // 2
    freqs = ROPE_BASE ** (-(jnp.arange(half, dtype=jnp.float32) * 2.0) / head_size)
    angles = jnp.arange(seq_len, dtype=jnp.float32)[:, None] * freqs[None, :]
    angles = jnp.concatenate([angles, angles], axis=1)
    return (jnp.cos(angles), jnp.sin(angles))


def rotate_half(vector):
    half = vector.shape[-1] // 2
    return jnp.concatenate([-vector[..., half:], vector[..., :half]], axis=-1)


def unrotate_half(vector):
    half = vector.shape[-1] // 2
    return jnp.concatenate([vector[..., half:], -vector[..., :half]], axis=-1)


def forward_pairs(
    tokens_in,
    lengths_here,
    norm_gain,
    final_gain,
    score_vector,
    query_weight,
    key_matrix,
    value_matrix,
    out_weight,
):
    pair_count, seq_len, model_width = tokens_in.shape
    head_count = query_weight.shape[1] // HEAD_WIDTH
    group_count = key_matrix.shape[1] // HEAD_WIDTH
    group_size = head_count // group_count
    inputs_wide = tokens_in.astype(jnp.float32)
    inv_rms = lax.rsqrt(jnp.mean(inputs_wide * inputs_wide, axis=-1, keepdims=True) + EPSILON)
    normed = (inputs_wide * inv_rms * norm_gain).astype(jnp.bfloat16)
    flat_rows = normed.reshape(pair_count * seq_len, model_width)
    key_proj = jnp.dot(flat_rows, key_matrix, preferred_element_type=jnp.float32).reshape(
        pair_count, seq_len, group_count, HEAD_WIDTH
    )
    value_proj = jnp.dot(flat_rows, value_matrix, preferred_element_type=jnp.float32).reshape(
        pair_count, seq_len, group_count, HEAD_WIDTH
    )
    positions = jnp.arange(seq_len, dtype=jnp.int32)
    last_index = lengths_here - 1
    onehot = (positions[None, :] == last_index[:, None]).astype(jnp.float32)
    normed_last = jnp.take_along_axis(normed, last_index[:, None, None], axis=1)[:, 0]
    query_proj = jnp.dot(normed_last, query_weight, preferred_element_type=jnp.float32).reshape(
        pair_count, head_count, HEAD_WIDTH
    )
    query_scale = lax.rsqrt(jnp.mean(query_proj * query_proj, axis=-1, keepdims=True) + EPSILON)
    query_unit = query_proj * query_scale
    key_scale = lax.rsqrt(jnp.mean(key_proj * key_proj, axis=-1, keepdims=True) + EPSILON)
    key_unit = key_proj * key_scale
    cos_table, sin_table = rope_tables(seq_len, HEAD_WIDTH)
    cos_query = jnp.dot(onehot, cos_table, precision=lax.Precision.HIGHEST)
    sin_query = jnp.dot(onehot, sin_table, precision=lax.Precision.HIGHEST)
    query_rot = (
        query_unit * cos_query[:, None, :] + rotate_half(query_unit) * sin_query[:, None, :]
    ).astype(jnp.bfloat16)
    key_rot = (
        key_unit * cos_table[None, :, None, :] + rotate_half(key_unit) * sin_table[None, :, None, :]
    ).astype(jnp.bfloat16)
    value_cast = value_proj.astype(jnp.bfloat16)
    grouped = query_rot.reshape(pair_count, group_count, group_size, HEAD_WIDTH)
    logits = jnp.einsum(
        "pkgd,pskd->pkgs", grouped, key_rot, preferred_element_type=jnp.float32
    ) * HEAD_WIDTH ** (-0.5)
    visible = (positions[None, :] <= last_index[:, None])[:, None, None, :]
    expos = jnp.where(visible, jnp.exp(logits), 0.0)
    attention_weights = expos / jnp.sum(expos, axis=-1, keepdims=True)
    probs_cast = attention_weights.astype(jnp.bfloat16)
    context = jnp.einsum(
        "pkgs,pskd->pkgd", probs_cast, value_cast, preferred_element_type=jnp.float32
    )
    context = context.astype(jnp.bfloat16).reshape(pair_count, head_count * HEAD_WIDTH)
    attended = jnp.dot(context, out_weight, preferred_element_type=jnp.float32)
    residual = jnp.take_along_axis(inputs_wide, last_index[:, None, None], axis=1)[:, 0] + attended
    out_scale = lax.rsqrt(jnp.mean(residual * residual, axis=-1, keepdims=True) + EPSILON)
    out_unit = residual * out_scale
    scores_here = jnp.sum(out_unit * final_gain * score_vector, axis=-1)
    stored = (
        tokens_in,
        onehot,
        inv_rms,
        normed,
        normed_last,
        query_unit,
        query_scale,
        key_unit,
        key_scale,
        cos_query,
        sin_query,
        cos_table,
        sin_table,
        query_rot,
        key_rot,
        value_cast,
        attention_weights,
        probs_cast,
        context,
        out_unit,
        out_scale,
    )
    return (scores_here, stored)


def backward_pairs(
    stored,
    grad_score,
    norm_gain,
    final_gain,
    score_vector,
    query_weight,
    key_matrix,
    value_matrix,
    out_weight,
):
    (
        tokens_in,
        onehot,
        inv_rms,
        normed,
        normed_last,
        query_unit,
        query_scale,
        key_unit,
        key_scale,
        cos_query,
        sin_query,
        cos_table,
        sin_table,
        query_rot,
        key_rot,
        value_cast,
        attention_weights,
        probs_cast,
        context,
        out_unit,
        out_scale,
    ) = stored
    pair_count, seq_len, model_width = tokens_in.shape
    head_count = query_weight.shape[1] // HEAD_WIDTH
    group_count = key_matrix.shape[1] // HEAD_WIDTH
    group_size = head_count // group_count
    grad_unit = grad_score[:, None] * score_vector * final_gain
    grad_resid = out_scale * (
        grad_unit - out_unit * jnp.mean(grad_unit * out_unit, axis=-1, keepdims=True)
    )
    grad_resid_cast = grad_resid.astype(jnp.bfloat16)
    grad_context = jnp.dot(
        grad_resid_cast, out_weight.T, preferred_element_type=jnp.float32
    ).astype(jnp.bfloat16)
    grad_context = grad_context.reshape(pair_count, group_count, group_size, HEAD_WIDTH)
    grad_probs = jnp.einsum(
        "pkgd,pskd->pkgs", grad_context, value_cast, preferred_element_type=jnp.float32
    )
    grad_vals = jnp.einsum(
        "pkgs,pkgd->pskd", probs_cast, grad_context, preferred_element_type=jnp.float32
    )
    spread = jnp.sum(attention_weights * grad_probs, axis=-1, keepdims=True)
    logit_gradient = (attention_weights * (grad_probs - spread)).astype(jnp.bfloat16)
    grouped = query_rot.reshape(pair_count, group_count, group_size, HEAD_WIDTH)
    rotated_query_gradient = jnp.einsum(
        "pkgs,pskd->pkgd", logit_gradient, key_rot, preferred_element_type=jnp.float32
    ) * HEAD_WIDTH ** (-0.5)
    rotated_query_gradient = rotated_query_gradient.reshape(pair_count, head_count, HEAD_WIDTH)
    grad_krot = jnp.einsum(
        "pkgs,pkgd->pskd", logit_gradient, grouped, preferred_element_type=jnp.float32
    ) * HEAD_WIDTH ** (-0.5)
    grad_qunit = rotated_query_gradient * cos_query[:, None, :] + unrotate_half(
        rotated_query_gradient * sin_query[:, None, :]
    )
    grad_kunit = grad_krot * cos_table[None, :, None, :] + unrotate_half(
        grad_krot * sin_table[None, :, None, :]
    )
    grad_qproj = query_scale * (
        grad_qunit - query_unit * jnp.mean(grad_qunit * query_unit, axis=-1, keepdims=True)
    )
    grad_kproj = key_scale * (
        grad_kunit - key_unit * jnp.mean(grad_kunit * key_unit, axis=-1, keepdims=True)
    )
    grad_q_cast = grad_qproj.reshape(pair_count, head_count * HEAD_WIDTH).astype(jnp.bfloat16)
    grad_k_cast = grad_kproj.reshape(pair_count * seq_len, group_count * HEAD_WIDTH).astype(
        jnp.bfloat16
    )
    grad_v_cast = grad_vals.reshape(pair_count * seq_len, group_count * HEAD_WIDTH).astype(
        jnp.bfloat16
    )
    flat_rows = normed.reshape(pair_count * seq_len, model_width)
    last_rows = jnp.concatenate([normed_last, grad_resid_cast, grad_q_cast, context], axis=1)
    grad_kv = jnp.dot(
        flat_rows.T,
        jnp.concatenate([grad_k_cast, grad_v_cast], axis=1),
        preferred_element_type=jnp.float32,
    )
    grad_normed = jnp.dot(grad_k_cast, key_matrix.T, preferred_element_type=jnp.float32)
    grad_normed = grad_normed + jnp.dot(
        grad_v_cast, value_matrix.T, preferred_element_type=jnp.float32
    )
    grad_normed = grad_normed.reshape(pair_count, seq_len, model_width)
    grad_last = jnp.dot(grad_q_cast, query_weight.T, preferred_element_type=jnp.float32)
    grad_normed = grad_normed + onehot[:, :, None] * grad_last[:, None, :]
    inputs_wide = tokens_in.astype(jnp.float32)
    grad_scaled = grad_normed * norm_gain
    grad_input = inv_rms * grad_scaled - inputs_wide * inv_rms * inv_rms * inv_rms * jnp.mean(
        grad_scaled * inputs_wide, axis=-1, keepdims=True
    )
    grad_input = grad_input + onehot[:, :, None] * grad_resid[:, None, :]
    return (grad_input.astype(jnp.bfloat16), last_rows, grad_kv)


class Place:
    def __init__(self):
        self.pb_count = lax.axis_size("pb")
        self.neg_count = lax.axis_size("neg")
        self.line_count = self.neg_count // 2
        self.pb = lax.axis_index("pb")
        neg = lax.axis_index("neg")
        self.line = neg // 2
        self.core = neg % 2
        self.partner = 1 - self.core

    def slot(self, pb, line, core):
        return pb * self.neg_count + line * 2 + core

    def line_peer(self, step):
        return lax.rem(self.line + step, self.line_count)

    def pb_peer(self, step):
        return lax.rem(self.pb + step, self.pb_count)

    def to_line(self, line):
        return (self.pb, line * 2 + self.core)

    def to_pb(self, pb):
        return (pb, self.line * 2 + self.core)

    def to_partner(self):
        return (self.pb, self.line * 2 + self.partner)

    def greet(self):
        barrier = pltpu.get_barrier_semaphore()
        targets = [self.to_line(self.line_peer(k)) for k in range(1, self.line_count)]
        targets += [self.to_pb(self.pb_peer(k)) for k in range(1, self.pb_count)]
        targets += [self.to_partner()]
        for target in targets:
            pl.semaphore_signal(barrier, inc=1, device_id=target, device_id_type=MESH_ID)
        pl.semaphore_wait(barrier, len(targets))


def remote(src, dst, send_sem, recv_sem, target):
    return pltpu.make_async_remote_copy(
        src_ref=src,
        dst_ref=dst,
        send_sem=send_sem,
        recv_sem=recv_sem,
        device_id=target,
        device_id_type=MESH_ID,
    )


def gather_sems(pb_count, neg_count):
    line_count = neg_count // 2
    return [
        pltpu.SemaphoreType.DMA((line_count,)),
        pltpu.SemaphoreType.DMA((line_count,)),
        pltpu.SemaphoreType.DMA((pb_count, line_count)),
        pltpu.SemaphoreType.DMA((pb_count, line_count)),
        pltpu.SemaphoreType.DMA((pb_count, line_count)),
        pltpu.SemaphoreType.DMA((pb_count, line_count)),
        pltpu.SemaphoreType.DMA,
    ]


class Gather:
    def __init__(self, place, own, full, sems):
        self.place, self.own, self.full = place, own, full
        self.line_send, self.line_recv, self.pb_send, self.pb_recv = sems[:4]
        self.core_send, self.core_recv, self.local_sem = sems[4:]
        self.sent = []

    def rows(self, pb, line, core):
        size = self.own.shape[0]
        start = self.place.slot(pb, line, core) * size
        return self.full.at[pl.ds(pl.multiple_of(start, size), size)]

    def send(self, src, dst, send_sem, recv_sem, target):
        copy = remote(src, dst, send_sem, recv_sem, target)
        copy.start()
        self.sent.append(copy)

    def spread(self, src, line):
        at = self.place
        dst = self.rows(at.pb, line, at.core)
        for k in range(1, at.pb_count):
            self.send(
                src, dst, self.pb_send.at[k, line], self.pb_recv.at[at.pb, line], at.to_pb(at.pb_peer(k))
            )
        self.pass_on(src, at.pb, line)

    def pass_on(self, src, pb, line):
        at = self.place
        dst = self.rows(pb, line, at.core)
        self.send(src, dst, self.core_send.at[pb, line], self.core_recv.at[pb, line], at.to_partner())

    def arrive(self, block, recv_sem):
        remote(block, block, self.local_sem, recv_sem, self.place.to_partner()).wait_recv()

    def start(self):
        at = self.place
        mine = self.rows(at.pb, at.line, at.core)
        self.local = pltpu.make_async_copy(self.own, mine, self.local_sem)
        self.local.start()
        for k in range(1, at.line_count):
            line = at.line_peer(k)
            self.send(
                self.own, mine, self.line_send.at[k], self.line_recv.at[at.line], at.to_line(line)
            )
        self.spread(self.own, at.line)

    def middle(self):
        at = self.place
        for k in range(1, at.line_count):
            line = at.line_peer(k)
            block = self.rows(at.pb, line, at.core)
            self.arrive(block, self.line_recv.at[line])
            self.spread(block, line)

    def finish(self):
        at = self.place
        for step in range(at.line_count):
            line = at.line_peer(step)
            for k in range(1, at.pb_count):
                pb = at.pb_peer(k)
                block = self.rows(pb, line, at.core)
                self.arrive(block, self.pb_recv.at[pb, line])
                self.pass_on(block, pb, line)
        for pb in range(at.pb_count):
            for line in range(at.line_count):
                self.arrive(self.rows(pb, line, at.partner), self.core_recv.at[pb, line])
        for copy in self.sent:
            copy.wait_send()
        self.local.wait()


def gather_kernel(own, full, *sems):
    place = Place()
    place.greet()
    gather = Gather(place, own, full, sems)
    gather.start()
    gather.middle()
    gather.finish()


VMEM_SPEC = pl.BlockSpec(memory_space=pltpu.VMEM)


def gather_weights(packed, pb_count, neg_count):
    return pl.pallas_call(
        gather_kernel,
        out_shape=jax.ShapeDtypeStruct(
            (packed.shape[0] * pb_count * neg_count, packed.shape[1]), packed.dtype
        ),
        in_specs=[VMEM_SPEC],
        out_specs=VMEM_SPEC,
        scratch_shapes=gather_sems(pb_count, neg_count),
        compiler_params=pltpu.CompilerParams(
            collective_id=0, has_side_effects=True, vmem_limit_bytes=32 * 2**20
        ),
    )(packed)


def listing_kernel(own, full, send, recv, local_sem):
    at = Place()
    barrier = pltpu.get_barrier_semaphore()
    neg = lax.axis_index("neg")
    peers = [lax.rem(neg + k, at.neg_count) for k in range(1, at.neg_count)]
    for peer in peers:
        pl.semaphore_signal(barrier, inc=1, device_id=(at.pb, peer), device_id_type=MESH_ID)
    pl.semaphore_wait(barrier, len(peers))
    copies = []
    local = pltpu.make_async_copy(own, full.at[neg], local_sem)
    local.start()
    for k, peer in enumerate(peers):
        copy = remote(own, full.at[neg], send.at[k], recv.at[neg], (at.pb, peer))
        copy.start()
        copies.append(copy)
    local.wait()
    for peer in peers:
        block = full.at[peer]
        remote(block, block, local_sem, recv.at[peer], (at.pb, peer)).wait_recv()
    for copy in copies:
        copy.wait_send()


def exchange_listing(own, neg_count):
    return pl.pallas_call(
        listing_kernel,
        out_shape=jax.ShapeDtypeStruct((neg_count,) + own.shape, own.dtype),
        in_specs=[VMEM_SPEC],
        out_specs=VMEM_SPEC,
        scratch_shapes=[
            pltpu.SemaphoreType.DMA((neg_count,)),
            pltpu.SemaphoreType.DMA((neg_count,)),
            pltpu.SemaphoreType.DMA,
        ],
        compiler_params=pltpu.CompilerParams(collective_id=1, has_side_effects=True),
    )(own)


def reduce_kernel(
    partial,
    last_rows,
    loss_row,
    reduced,
    all_rows,
    all_losses,
    from_core,
    paired,
    from_pb,
    summed,
    from_line,
    core_send,
    core_recv,
    pb_send,
    pb_recv,
    line_send,
    line_recv,
    loss_send,
    loss_recv,
    loss_local,
    *sems,
):
    at = Place()
    at.greet()
    gather = Gather(at, last_rows, all_rows, sems)
    copies = []

    def send(src, dst, send_sem, recv_sem, target):
        copy = remote(src, dst, send_sem, recv_sem, target)
        copy.start()
        copies.append(copy)

    def arrive(block, recv_sem):
        remote(block, block, loss_local, recv_sem, at.to_partner()).wait_recv()

    for k in range(1, at.pb_count + 1):
        pb = at.pb_peer(k % at.pb_count)
        send(
            partial.at[pb, :, at.partner],
            from_core.at[pb],
            core_send.at[pb],
            core_recv.at[pb],
            at.to_partner(),
        )
    gather.start()
    local = pltpu.make_async_copy(loss_row, all_losses.at[at.pb], loss_local)
    local.start()
    for k in range(1, at.pb_count):
        send(
            loss_row, all_losses.at[at.pb], loss_send.at[k], loss_recv.at[at.pb], at.to_pb(at.pb_peer(k))
        )
    for k in range(1, at.pb_count + 1):
        pb = at.pb_peer(k % at.pb_count)
        arrive(from_core.at[pb], core_recv.at[pb])
        both = partial[pb, :, at.core].astype(jnp.float32) + from_core[pb].astype(jnp.float32)
        paired[pb] = both.astype(jnp.bfloat16)
        if k < at.pb_count:
            send(
                paired.at[pb], from_pb.at[at.pb], pb_send.at[k], pb_recv.at[at.pb], at.to_pb(pb)
            )
    gather.middle()
    for k in range(1, at.pb_count):
        pb = at.pb_peer(k)
        arrive(from_pb.at[pb], pb_recv.at[pb])
    for step in range(1, at.line_count + 1):
        line = at.line_peer(step % at.line_count)
        total = paired[at.pb, line].astype(jnp.float32)
        for k in range(1, at.pb_count):
            total = total + from_pb[at.pb_peer(k), line].astype(jnp.float32)
        if step < at.line_count:
            summed[line] = total.astype(jnp.bfloat16)
            send(
                summed.at[line],
                from_line.at[at.line],
                line_send.at[line],
                line_recv.at[at.line],
                at.to_line(line),
            )
    for step in range(1, at.line_count):
        line = at.line_peer(step)
        arrive(from_line.at[line], line_recv.at[line])
        total = total + from_line[line].astype(jnp.float32)
    reduced[...] = total
    gather.finish()
    local.wait()
    for k in range(1, at.pb_count):
        pb = at.pb_peer(k)
        arrive(all_losses.at[pb], loss_recv.at[pb])
    for copy in copies:
        copy.wait_send()


def reduce_gradients(grad_kv, last_rows, loss_row, pb_count, neg_count):
    line_count = neg_count // 2
    share = grad_kv.shape[0] // (pb_count * neg_count)
    width = grad_kv.shape[1]
    partial = grad_kv.reshape(pb_count, line_count, 2, share, width)
    block = (pb_count, line_count, share, width)
    dma = pltpu.SemaphoreType.DMA
    return pl.pallas_call(
        reduce_kernel,
        out_shape=(
            jax.ShapeDtypeStruct((share, width), jnp.float32),
            jax.ShapeDtypeStruct((last_rows.shape[0] * pb_count * neg_count, last_rows.shape[1]), last_rows.dtype),
            jax.ShapeDtypeStruct((pb_count,) + loss_row.shape, loss_row.dtype),
        ),
        in_specs=[VMEM_SPEC] * 3,
        out_specs=(VMEM_SPEC,) * 3,
        scratch_shapes=[
            pltpu.VMEM(block, jnp.bfloat16),
            pltpu.VMEM(block, jnp.bfloat16),
            pltpu.VMEM(block, jnp.bfloat16),
            pltpu.VMEM(block[1:], jnp.bfloat16),
            pltpu.VMEM(block[1:], jnp.bfloat16),
            dma((pb_count,)),
            dma((pb_count,)),
            dma((pb_count,)),
            dma((pb_count,)),
            dma((line_count,)),
            dma((line_count,)),
            dma((pb_count,)),
            dma((pb_count,)),
            dma,
        ]
        + gather_sems(pb_count, neg_count),
        compiler_params=pltpu.CompilerParams(
            collective_id=2, has_side_effects=True, vmem_limit_bytes=40 * 2**20
        ),
    )(partial, last_rows, loss_row)


def shards(
    hidden,
    lengths,
    teacher,
    norm_gain,
    final_gain,
    score_vector,
    query_weight,
    key_matrix,
    value_matrix,
    out_weight,
):
    both = ("pb", "neg")
    width = query_weight.shape[1]
    kv_width = key_matrix.shape[1]
    head_width = out_weight.shape[0]
    packed = jnp.concatenate([query_weight, key_matrix, value_matrix, out_weight.T], axis=1)
    pb_count, neg_count = lax.axis_size("pb"), lax.axis_size("neg")
    own_kernels = packed.shape[0] % 16 == 0 and neg_count % 2 == 0
    if own_kernels:
        everything = gather_weights(packed, pb_count, neg_count)
    else:
        everything = lax.all_gather(packed, both, axis=0, tiled=True)
    full_query = everything[:, :width]
    full_key = everything[:, width : width + kv_width]
    full_value = everything[:, width + kv_width : width + 2 * kv_width]
    full_out_t = everything[:, width + 2 * kv_width :]
    scores_here, stored = forward_pairs(
        hidden[0],
        lengths[0],
        norm_gain,
        final_gain,
        score_vector,
        full_query,
        full_key,
        full_value,
        full_out_t.T,
    )
    pair_count = scores_here.shape[0]
    row = lax.axis_index("pb")
    listing = jnp.concatenate([scores_here, teacher[0]])[None]
    if own_kernels:
        lanes = jnp.pad(listing, ((0, 0), (0, HEAD_WIDTH - 2 * pair_count)))
        listed = exchange_listing(lanes, neg_count)[:, 0, : 2 * pair_count]
    else:
        listed = lax.all_gather(listing, "neg", axis=0, tiled=True)
    all_scores = listed[:, :pair_count]
    all_scaled = listed[:, pair_count:] / TEACHER_TEMP
    my_total_s = jnp.sum(jnp.exp(all_scores))
    expo_t = jnp.exp(all_scaled)
    my_total_t = jnp.sum(expo_t)
    loss_here = jnp.sum(
        expo_t
        / my_total_t
        * (all_scaled - jnp.log(my_total_t) - (all_scores - jnp.log(my_total_s)))
    )
    prob_s = jnp.exp(scores_here) / my_total_s
    prob_t = jnp.exp(teacher[0] / TEACHER_TEMP) / my_total_t
    grad_score = GRAD_SCALE * (prob_s - prob_t)
    grad_input, last_rows, grad_kv = backward_pairs(
        stored,
        grad_score,
        norm_gain,
        final_gain,
        score_vector,
        full_query,
        full_key,
        full_value,
        full_out_t.T,
    )
    grad_kv = grad_kv.astype(jnp.bfloat16)
    if own_kernels:
        spaced = jnp.pad(last_rows.reshape(pair_count * 4, -1), ((0, -pair_count * 4 % 16), (0, 0)))
        reduced, rows, losses = reduce_gradients(
            grad_kv, spaced, jnp.full((1, HEAD_WIDTH), loss_here), pb_count, neg_count
        )
        rows = rows.reshape(-1, spaced.shape[0], spaced.shape[1])[:, : pair_count * 4]
        rows = rows.reshape(pb_count * neg_count * pair_count, -1)
        loss_value = jnp.sum(losses[:, 0, 0])
    else:
        reduced = lax.psum_scatter(grad_kv, both, scatter_dimension=0, tiled=True)
        reduced = reduced.astype(jnp.float32)
        rows = lax.all_gather(last_rows, both, axis=0, tiled=True)
        loss_value = lax.psum(loss_here, "pb")
    index = row * lax.axis_size("neg") + lax.axis_index("neg")
    share = query_weight.shape[0]
    model_width = share * lax.axis_size("pb") * lax.axis_size("neg")
    out_share = out_weight.shape[1]
    normed_cols = lax.dynamic_slice_in_dim(rows, index * share, share, axis=1)
    resid_cols = lax.dynamic_slice_in_dim(rows, model_width + index * out_share, out_share, axis=1)
    rest = 2 * model_width
    all_q = rows[:, rest : rest + width]
    all_context = rows[:, rest + width :]
    grad_query = jnp.dot(normed_cols.T, all_q, preferred_element_type=jnp.float32)
    grad_out = jnp.dot(all_context.T, resid_cols, preferred_element_type=jnp.float32)
    return (
        scores_here[None],
        loss_value,
        grad_input[None],
        grad_query,
        reduced[:, :kv_width],
        reduced[:, kv_width:],
        grad_out,
    )


def solution(mesh):
    placed = (
        P("pb", "neg", None, None),
        P("pb", "neg"),
        P("pb", "neg"),
        P(),
        P(),
        P(),
        P(("pb", "neg"), None),
        P(("pb", "neg"), None),
        P(("pb", "neg"), None),
        P(None, ("pb", "neg")),
    )
    return jax.shard_map(
        shards,
        mesh=mesh,
        in_specs=placed,
        out_specs=(
            P("pb", "neg"),
            P(),
            P("pb", "neg", None, None),
            P(("pb", "neg"), None),
            P(("pb", "neg"), None),
            P(("pb", "neg"), None),
            P(None, ("pb", "neg")),
        ),
        check_vma=False,
    )
```

```python
import functools

import jax
import jax.numpy as jnp
from jax import lax
from jax.experimental import pallas as pl
from jax.experimental.pallas import tpu as pltpu
from jax.sharding import PartitionSpec as P

HEAD_WIDTH = 128
MESH_ID = pl.DeviceIdType.MESH

EPSILON = 1e-06
ROPE_BASE = 1000000.0
TEACHER_TEMP = 2.0
GRAD_SCALE = 512.0


def rope_tables(seq_len, head_size):
    half = head_size // 2
    freqs = ROPE_BASE ** (-(jnp.arange(half, dtype=jnp.float32) * 2.0) / head_size)
    angles = jnp.arange(seq_len, dtype=jnp.float32)[:, None] * freqs[None, :]
    angles = jnp.concatenate([angles, angles], axis=1)
    return (jnp.cos(angles), jnp.sin(angles))


def rotate_half(vector):
    half = vector.shape[-1] // 2
    return jnp.concatenate([-vector[..., half:], vector[..., :half]], axis=-1)


def unrotate_half(vector):
    half = vector.shape[-1] // 2
    return jnp.concatenate([vector[..., half:], -vector[..., :half]], axis=-1)


def forward_pairs(
    tokens_in,
    lengths_here,
    norm_gain,
    final_gain,
    score_vector,
    query_weight,
    key_matrix,
    value_matrix,
    out_weight,
):
    pair_count, seq_len, model_width = tokens_in.shape
    head_count = query_weight.shape[1] // HEAD_WIDTH
    group_count = key_matrix.shape[1] // HEAD_WIDTH
    group_size = head_count // group_count
    inputs_wide = tokens_in.astype(jnp.float32)
    inv_rms = lax.rsqrt(jnp.mean(inputs_wide * inputs_wide, axis=-1, keepdims=True) + EPSILON)
    normed = (inputs_wide * inv_rms * norm_gain).astype(jnp.bfloat16)
    flat_rows = normed.reshape(pair_count * seq_len, model_width)
    key_proj = jnp.dot(flat_rows, key_matrix, preferred_element_type=jnp.float32).reshape(
        pair_count, seq_len, group_count, HEAD_WIDTH
    )
    value_proj = jnp.dot(flat_rows, value_matrix, preferred_element_type=jnp.float32).reshape(
        pair_count, seq_len, group_count, HEAD_WIDTH
    )
    positions = jnp.arange(seq_len, dtype=jnp.int32)
    last_index = lengths_here - 1
    onehot = (positions[None, :] == last_index[:, None]).astype(jnp.float32)
    normed_last = jnp.take_along_axis(normed, last_index[:, None, None], axis=1)[:, 0]
    query_proj = jnp.dot(normed_last, query_weight, preferred_element_type=jnp.float32).reshape(
        pair_count, head_count, HEAD_WIDTH
    )
    query_scale = lax.rsqrt(jnp.mean(query_proj * query_proj, axis=-1, keepdims=True) + EPSILON)
    query_unit = query_proj * query_scale
    key_scale = lax.rsqrt(jnp.mean(key_proj * key_proj, axis=-1, keepdims=True) + EPSILON)
    key_unit = key_proj * key_scale
    cos_table, sin_table = rope_tables(seq_len, HEAD_WIDTH)
    cos_query = jnp.dot(onehot, cos_table, precision=lax.Precision.HIGHEST)
    sin_query = jnp.dot(onehot, sin_table, precision=lax.Precision.HIGHEST)
    query_rot = (
        query_unit * cos_query[:, None, :] + rotate_half(query_unit) * sin_query[:, None, :]
    ).astype(jnp.bfloat16)
    key_rot = (
        key_unit * cos_table[None, :, None, :] + rotate_half(key_unit) * sin_table[None, :, None, :]
    ).astype(jnp.bfloat16)
    value_cast = value_proj.astype(jnp.bfloat16)
    grouped = query_rot.reshape(pair_count, group_count, group_size, HEAD_WIDTH)
    logits = jnp.einsum(
        "pkgd,pskd->pkgs", grouped, key_rot, preferred_element_type=jnp.float32
    ) * HEAD_WIDTH ** (-0.5)
    visible = (positions[None, :] <= last_index[:, None])[:, None, None, :]
    expos = jnp.where(visible, jnp.exp(logits), 0.0)
    attention_weights = expos / jnp.sum(expos, axis=-1, keepdims=True)
    probs_cast = attention_weights.astype(jnp.bfloat16)
    context = jnp.einsum(
        "pkgs,pskd->pkgd", probs_cast, value_cast, preferred_element_type=jnp.float32
    )
    context = context.astype(jnp.bfloat16).reshape(pair_count, head_count * HEAD_WIDTH)
    attended = jnp.dot(context, out_weight, preferred_element_type=jnp.float32)
    residual = jnp.take_along_axis(inputs_wide, last_index[:, None, None], axis=1)[:, 0] + attended
    out_scale = lax.rsqrt(jnp.mean(residual * residual, axis=-1, keepdims=True) + EPSILON)
    out_unit = residual * out_scale
    scores_here = jnp.sum(out_unit * final_gain * score_vector, axis=-1)
    stored = (
        tokens_in,
        onehot,
        inv_rms,
        normed,
        normed_last,
        query_unit,
        query_scale,
        key_unit,
        key_scale,
        cos_query,
        sin_query,
        cos_table,
        sin_table,
        query_rot,
        key_rot,
        value_cast,
        attention_weights,
        probs_cast,
        context,
        out_unit,
        out_scale,
    )
    return (scores_here, stored)


def backward_pairs(
    stored,
    grad_score,
    norm_gain,
    final_gain,
    score_vector,
    query_weight,
    key_matrix,
    value_matrix,
    out_weight,
):
    (
        tokens_in,
        onehot,
        inv_rms,
        normed,
        normed_last,
        query_unit,
        query_scale,
        key_unit,
        key_scale,
        cos_query,
        sin_query,
        cos_table,
        sin_table,
        query_rot,
        key_rot,
        value_cast,
        attention_weights,
        probs_cast,
        context,
        out_unit,
        out_scale,
    ) = stored
    pair_count, seq_len, model_width = tokens_in.shape
    head_count = query_weight.shape[1] // HEAD_WIDTH
    group_count = key_matrix.shape[1] // HEAD_WIDTH
    group_size = head_count // group_count
    grad_unit = grad_score[:, None] * score_vector * final_gain
    grad_resid = out_scale * (
        grad_unit - out_unit * jnp.mean(grad_unit * out_unit, axis=-1, keepdims=True)
    )
    grad_resid_cast = grad_resid.astype(jnp.bfloat16)
    grad_context = jnp.dot(
        grad_resid_cast, out_weight.T, preferred_element_type=jnp.float32
    ).astype(jnp.bfloat16)
    grad_context = grad_context.reshape(pair_count, group_count, group_size, HEAD_WIDTH)
    grad_probs = jnp.einsum(
        "pkgd,pskd->pkgs", grad_context, value_cast, preferred_element_type=jnp.float32
    )
    grad_vals = jnp.einsum(
        "pkgs,pkgd->pskd", probs_cast, grad_context, preferred_element_type=jnp.float32
    )
    spread = jnp.sum(attention_weights * grad_probs, axis=-1, keepdims=True)
    logit_gradient = (attention_weights * (grad_probs - spread)).astype(jnp.bfloat16)
    grouped = query_rot.reshape(pair_count, group_count, group_size, HEAD_WIDTH)
    rotated_query_gradient = jnp.einsum(
        "pkgs,pskd->pkgd", logit_gradient, key_rot, preferred_element_type=jnp.float32
    ) * HEAD_WIDTH ** (-0.5)
    rotated_query_gradient = rotated_query_gradient.reshape(pair_count, head_count, HEAD_WIDTH)
    grad_krot = jnp.einsum(
        "pkgs,pkgd->pskd", logit_gradient, grouped, preferred_element_type=jnp.float32
    ) * HEAD_WIDTH ** (-0.5)
    grad_qunit = rotated_query_gradient * cos_query[:, None, :] + unrotate_half(
        rotated_query_gradient * sin_query[:, None, :]
    )
    grad_kunit = grad_krot * cos_table[None, :, None, :] + unrotate_half(
        grad_krot * sin_table[None, :, None, :]
    )
    grad_qproj = query_scale * (
        grad_qunit - query_unit * jnp.mean(grad_qunit * query_unit, axis=-1, keepdims=True)
    )
    grad_kproj = key_scale * (
        grad_kunit - key_unit * jnp.mean(grad_kunit * key_unit, axis=-1, keepdims=True)
    )
    grad_q_cast = grad_qproj.reshape(pair_count, head_count * HEAD_WIDTH).astype(jnp.bfloat16)
    grad_k_cast = grad_kproj.reshape(pair_count * seq_len, group_count * HEAD_WIDTH).astype(
        jnp.bfloat16
    )
    grad_v_cast = grad_vals.reshape(pair_count * seq_len, group_count * HEAD_WIDTH).astype(
        jnp.bfloat16
    )
    flat_rows = normed.reshape(pair_count * seq_len, model_width)
    last_rows = jnp.concatenate([normed_last, grad_resid_cast, grad_q_cast, context], axis=1)
    grad_kv = jnp.dot(
        flat_rows.T,
        jnp.concatenate([grad_k_cast, grad_v_cast], axis=1),
        preferred_element_type=jnp.float32,
    )
    grad_normed = jnp.dot(grad_k_cast, key_matrix.T, preferred_element_type=jnp.float32)
    grad_normed = grad_normed + jnp.dot(
        grad_v_cast, value_matrix.T, preferred_element_type=jnp.float32
    )
    grad_normed = grad_normed.reshape(pair_count, seq_len, model_width)
    grad_last = jnp.dot(grad_q_cast, query_weight.T, preferred_element_type=jnp.float32)
    grad_normed = grad_normed + onehot[:, :, None] * grad_last[:, None, :]
    inputs_wide = tokens_in.astype(jnp.float32)
    grad_scaled = grad_normed * norm_gain
    grad_input = inv_rms * grad_scaled - inputs_wide * inv_rms * inv_rms * inv_rms * jnp.mean(
        grad_scaled * inputs_wide, axis=-1, keepdims=True
    )
    grad_input = grad_input + onehot[:, :, None] * grad_resid[:, None, :]
    return (grad_input.astype(jnp.bfloat16), last_rows, grad_kv)


class Place:
    def __init__(self):
        self.pb_count = lax.axis_size("pb")
        self.neg_count = lax.axis_size("neg")
        self.line_count = self.neg_count // 2
        self.pb = lax.axis_index("pb")
        neg = lax.axis_index("neg")
        self.line = neg // 2
        self.core = neg % 2
        self.partner = 1 - self.core

    def slot(self, pb, line, core):
        return pb * self.neg_count + line * 2 + core

    def line_peer(self, step):
        return lax.rem(self.line + step, self.line_count)

    def pb_peer(self, step):
        return lax.rem(self.pb + step, self.pb_count)

    def to_line(self, line):
        return (self.pb, line * 2 + self.core)

    def to_pb(self, pb):
        return (pb, self.line * 2 + self.core)

    def to_partner(self):
        return (self.pb, self.line * 2 + self.partner)

    def greet(self):
        barrier = pltpu.get_barrier_semaphore()
        targets = [self.to_line(self.line_peer(k)) for k in range(1, self.line_count)]
        targets += [self.to_pb(self.pb_peer(k)) for k in range(1, self.pb_count)]
        targets += [self.to_partner()]
        for target in targets:
            pl.semaphore_signal(barrier, inc=1, device_id=target, device_id_type=MESH_ID)
        pl.semaphore_wait(barrier, len(targets))


def remote(src, dst, send_sem, recv_sem, target):
    return pltpu.make_async_remote_copy(
        src_ref=src,
        dst_ref=dst,
        send_sem=send_sem,
        recv_sem=recv_sem,
        device_id=target,
        device_id_type=MESH_ID,
    )


def gather_sems(pb_count, neg_count):
    line_count = neg_count // 2
    return [
        pltpu.SemaphoreType.DMA((line_count,)),
        pltpu.SemaphoreType.DMA((line_count,)),
        pltpu.SemaphoreType.DMA((2, line_count)),
        pltpu.SemaphoreType.DMA((2, line_count)),
        pltpu.SemaphoreType.DMA((2, line_count)),
        pltpu.SemaphoreType.DMA((2, line_count)),
        pltpu.SemaphoreType.DMA((pb_count, line_count)),
        pltpu.SemaphoreType.DMA((pb_count, line_count)),
        pltpu.SemaphoreType.DMA,
    ]


class Gather:
    def __init__(self, place, own, full, sems):
        self.place, self.own, self.full = place, own, full
        self.line_send, self.line_recv, self.pb_send, self.pb_recv = sems[:4]
        self.half_send, self.half_recv = sems[4:6]
        self.core_send, self.core_recv, self.local_sem = sems[6:]
        self.sent = []
        across = place.pb + 1 - 2 * (place.pb % 2)
        along = place.pb + 2 - 4 * (place.pb // 2)
        self.near = (across, along)
        self.corner = 3 - place.pb

    def rows(self, pb, line, core):
        size = self.own.shape[0]
        start = self.place.slot(pb, line, core) * size
        return self.full.at[pl.ds(pl.multiple_of(start, size), size)]

    def send(self, src, dst, send_sem, recv_sem, target):
        copy = remote(src, dst, send_sem, recv_sem, target)
        copy.start()
        self.sent.append(copy)

    def spread(self, src, line):
        at = self.place
        dst = self.rows(at.pb, line, at.core)
        for side in range(2):
            self.send(
                src, dst, self.pb_send.at[side, line], self.pb_recv.at[side, line], at.to_pb(self.near[side])
            )
        self.pass_on(src, at.pb, line)

    def pass_on(self, src, pb, line):
        at = self.place
        dst = self.rows(pb, line, at.core)
        self.send(src, dst, self.core_send.at[pb, line], self.core_recv.at[pb, line], at.to_partner())

    def arrive(self, block, recv_sem):
        remote(block, block, self.local_sem, recv_sem, self.place.to_partner()).wait_recv()

    def start(self):
        at = self.place
        mine = self.rows(at.pb, at.line, at.core)
        self.local = pltpu.make_async_copy(self.own, mine, self.local_sem)
        self.local.start()
        for k in range(1, at.line_count):
            line = at.line_peer(k)
            self.send(
                self.own, mine, self.line_send.at[k], self.line_recv.at[at.line], at.to_line(line)
            )
        self.spread(self.own, at.line)

    def middle(self):
        at = self.place
        for k in range(1, at.line_count):
            line = at.line_peer(k)
            block = self.rows(at.pb, line, at.core)
            self.arrive(block, self.line_recv.at[line])
            self.spread(block, line)

    def half(self, block, side):
        width = block.shape[1] // 2
        return block.at[:, pl.ds(side * width, width)]

    def relay(self):
        at = self.place
        for step in range(at.line_count):
            line = at.line_peer(step)
            for side in range(2):
                block = self.rows(self.near[side], line, at.core)
                self.arrive(block, self.pb_recv.at[side, line])
                part = self.half(block, side)
                self.send(
                    part,
                    part,
                    self.half_send.at[side, line],
                    self.half_recv.at[side, line],
                    at.to_pb(self.near[1 - side]),
                )
                self.pass_on(block, self.near[side], line)

    def finish(self):
        at = self.place
        for step in range(at.line_count):
            line = at.line_peer(step)
            block = self.rows(self.corner, line, at.core)
            for side in range(2):
                self.arrive(self.half(block, side), self.half_recv.at[side, line])
            self.pass_on(block, self.corner, line)
        for pb in range(at.pb_count):
            for line in range(at.line_count):
                self.arrive(self.rows(pb, line, at.partner), self.core_recv.at[pb, line])
        for copy in self.sent:
            copy.wait_send()
        self.local.wait()


def gather_kernel(count, *refs):
    place = Place()
    place.greet()
    owns, fulls, sems = refs[:count], refs[count : 2 * count], refs[2 * count :]
    each = len(sems) // count
    gathers = [
        Gather(place, owns[i], fulls[i], sems[i * each : (i + 1) * each]) for i in range(count)
    ]
    for gather in gathers:
        gather.start()
    for gather in gathers:
        gather.middle()
    for gather in gathers:
        gather.relay()
    for gather in gathers:
        gather.finish()


VMEM_SPEC = pl.BlockSpec(memory_space=pltpu.VMEM)


def gather_weights(shares, pb_count, neg_count):
    count = len(shares)
    return pl.pallas_call(
        functools.partial(gather_kernel, count),
        out_shape=tuple(
            jax.ShapeDtypeStruct((w.shape[0] * pb_count * neg_count, w.shape[1]), w.dtype)
            for w in shares
        ),
        in_specs=[VMEM_SPEC] * count,
        out_specs=(VMEM_SPEC,) * count,
        scratch_shapes=gather_sems(pb_count, neg_count) * count,
        compiler_params=pltpu.CompilerParams(
            collective_id=0, has_side_effects=True, vmem_limit_bytes=32 * 2**20
        ),
    )(*shares)


def listing_kernel(own, full, send, recv, local_sem):
    at = Place()
    barrier = pltpu.get_barrier_semaphore()
    neg = lax.axis_index("neg")
    peers = [lax.rem(neg + k, at.neg_count) for k in range(1, at.neg_count)]
    for peer in peers:
        pl.semaphore_signal(barrier, inc=1, device_id=(at.pb, peer), device_id_type=MESH_ID)
    pl.semaphore_wait(barrier, len(peers))
    copies = []
    local = pltpu.make_async_copy(own, full.at[neg], local_sem)
    local.start()
    for k, peer in enumerate(peers):
        copy = remote(own, full.at[neg], send.at[k], recv.at[neg], (at.pb, peer))
        copy.start()
        copies.append(copy)
    local.wait()
    for peer in peers:
        block = full.at[peer]
        remote(block, block, local_sem, recv.at[peer], (at.pb, peer)).wait_recv()
    for copy in copies:
        copy.wait_send()


def exchange_listing(own, neg_count):
    return pl.pallas_call(
        listing_kernel,
        out_shape=jax.ShapeDtypeStruct((neg_count,) + own.shape, own.dtype),
        in_specs=[VMEM_SPEC],
        out_specs=VMEM_SPEC,
        scratch_shapes=[
            pltpu.SemaphoreType.DMA((neg_count,)),
            pltpu.SemaphoreType.DMA((neg_count,)),
            pltpu.SemaphoreType.DMA,
        ],
        compiler_params=pltpu.CompilerParams(collective_id=1, has_side_effects=True),
    )(own)


def reduce_kernel(
    partial,
    last_rows,
    loss_row,
    reduced,
    all_rows,
    all_losses,
    from_core,
    paired,
    from_pb,
    summed,
    from_line,
    core_send,
    core_recv,
    pb_send,
    pb_recv,
    line_send,
    line_recv,
    loss_send,
    loss_recv,
    loss_local,
    *sems,
):
    at = Place()
    at.greet()
    gather = Gather(at, last_rows, all_rows, sems)
    copies = []

    def send(src, dst, send_sem, recv_sem, target):
        copy = remote(src, dst, send_sem, recv_sem, target)
        copy.start()
        copies.append(copy)

    def arrive(block, recv_sem):
        remote(block, block, loss_local, recv_sem, at.to_partner()).wait_recv()

    for k in range(1, at.pb_count + 1):
        pb = at.pb_peer(k % at.pb_count)
        send(
            partial.at[pb, :, at.partner],
            from_core.at[pb],
            core_send.at[pb],
            core_recv.at[pb],
            at.to_partner(),
        )
    gather.start()
    local = pltpu.make_async_copy(loss_row, all_losses.at[at.pb], loss_local)
    local.start()
    for k in range(1, at.pb_count):
        send(
            loss_row, all_losses.at[at.pb], loss_send.at[k], loss_recv.at[at.pb], at.to_pb(at.pb_peer(k))
        )
    for k in range(1, at.pb_count + 1):
        pb = at.pb_peer(k % at.pb_count)
        arrive(from_core.at[pb], core_recv.at[pb])
        both = partial[pb, :, at.core].astype(jnp.float32) + from_core[pb].astype(jnp.float32)
        paired[pb] = both.astype(jnp.bfloat16)
        if k < at.pb_count:
            send(
                paired.at[pb], from_pb.at[at.pb], pb_send.at[k], pb_recv.at[at.pb], at.to_pb(pb)
            )
    gather.middle()
    gather.relay()
    for k in range(1, at.pb_count):
        pb = at.pb_peer(k)
        arrive(from_pb.at[pb], pb_recv.at[pb])
    for step in range(1, at.line_count + 1):
        line = at.line_peer(step % at.line_count)
        total = paired[at.pb, line].astype(jnp.float32)
        for k in range(1, at.pb_count):
            total = total + from_pb[at.pb_peer(k), line].astype(jnp.float32)
        if step < at.line_count:
            summed[line] = total.astype(jnp.bfloat16)
            send(
                summed.at[line],
                from_line.at[at.line],
                line_send.at[line],
                line_recv.at[at.line],
                at.to_line(line),
            )
    for step in range(1, at.line_count):
        line = at.line_peer(step)
        arrive(from_line.at[line], line_recv.at[line])
        total = total + from_line[line].astype(jnp.float32)
    reduced[...] = total
    gather.finish()
    local.wait()
    for k in range(1, at.pb_count):
        pb = at.pb_peer(k)
        arrive(all_losses.at[pb], loss_recv.at[pb])
    for copy in copies:
        copy.wait_send()


def reduce_gradients(grad_kv, last_rows, loss_row, pb_count, neg_count):
    line_count = neg_count // 2
    share = grad_kv.shape[0] // (pb_count * neg_count)
    width = grad_kv.shape[1]
    partial = grad_kv.reshape(pb_count, line_count, 2, share, width)
    block = (pb_count, line_count, share, width)
    dma = pltpu.SemaphoreType.DMA
    return pl.pallas_call(
        reduce_kernel,
        out_shape=(
            jax.ShapeDtypeStruct((share, width), jnp.float32),
            jax.ShapeDtypeStruct((last_rows.shape[0] * pb_count * neg_count, last_rows.shape[1]), last_rows.dtype),
            jax.ShapeDtypeStruct((pb_count,) + loss_row.shape, loss_row.dtype),
        ),
        in_specs=[VMEM_SPEC] * 3,
        out_specs=(VMEM_SPEC,) * 3,
        scratch_shapes=[
            pltpu.VMEM(block, jnp.bfloat16),
            pltpu.VMEM(block, jnp.bfloat16),
            pltpu.VMEM(block, jnp.bfloat16),
            pltpu.VMEM(block[1:], jnp.bfloat16),
            pltpu.VMEM(block[1:], jnp.bfloat16),
            dma((pb_count,)),
            dma((pb_count,)),
            dma((pb_count,)),
            dma((pb_count,)),
            dma((line_count,)),
            dma((line_count,)),
            dma((pb_count,)),
            dma((pb_count,)),
            dma,
        ]
        + gather_sems(pb_count, neg_count),
        compiler_params=pltpu.CompilerParams(
            collective_id=2, has_side_effects=True, vmem_limit_bytes=40 * 2**20
        ),
    )(partial, last_rows, loss_row)


def shards(
    hidden,
    lengths,
    teacher,
    norm_gain,
    final_gain,
    score_vector,
    query_weight,
    key_matrix,
    value_matrix,
    out_weight,
):
    both = ("pb", "neg")
    width = query_weight.shape[1]
    kv_width = key_matrix.shape[1]
    shares = (query_weight, key_matrix, value_matrix, out_weight.T)
    pb_count, neg_count = lax.axis_size("pb"), lax.axis_size("neg")
    even = all(w.shape[0] % 16 == 0 and w.shape[1] % (2 * HEAD_WIDTH) == 0 for w in shares)
    own_kernels = even and pb_count == 4 and neg_count % 2 == 0
    if own_kernels:
        full_query, full_key, full_value, full_out_t = gather_weights(shares, pb_count, neg_count)
    else:
        packed = jnp.concatenate(shares, axis=1)
        everything = lax.all_gather(packed, both, axis=0, tiled=True)
        full_query = everything[:, :width]
        full_key = everything[:, width : width + kv_width]
        full_value = everything[:, width + kv_width : width + 2 * kv_width]
        full_out_t = everything[:, width + 2 * kv_width :]
    scores_here, stored = forward_pairs(
        hidden[0],
        lengths[0],
        norm_gain,
        final_gain,
        score_vector,
        full_query,
        full_key,
        full_value,
        full_out_t.T,
    )
    pair_count = scores_here.shape[0]
    row = lax.axis_index("pb")
    listing = jnp.concatenate([scores_here, teacher[0]])[None]
    if own_kernels:
        lanes = jnp.pad(listing, ((0, 0), (0, HEAD_WIDTH - 2 * pair_count)))
        listed = exchange_listing(lanes, neg_count)[:, 0, : 2 * pair_count]
    else:
        listed = lax.all_gather(listing, "neg", axis=0, tiled=True)
    all_scores = listed[:, :pair_count]
    all_scaled = listed[:, pair_count:] / TEACHER_TEMP
    my_total_s = jnp.sum(jnp.exp(all_scores))
    expo_t = jnp.exp(all_scaled)
    my_total_t = jnp.sum(expo_t)
    loss_here = jnp.sum(
        expo_t
        / my_total_t
        * (all_scaled - jnp.log(my_total_t) - (all_scores - jnp.log(my_total_s)))
    )
    prob_s = jnp.exp(scores_here) / my_total_s
    prob_t = jnp.exp(teacher[0] / TEACHER_TEMP) / my_total_t
    grad_score = GRAD_SCALE * (prob_s - prob_t)
    grad_input, last_rows, grad_kv = backward_pairs(
        stored,
        grad_score,
        norm_gain,
        final_gain,
        score_vector,
        full_query,
        full_key,
        full_value,
        full_out_t.T,
    )
    grad_kv = grad_kv.astype(jnp.bfloat16)
    if own_kernels:
        spaced = jnp.pad(last_rows.reshape(pair_count * 4, -1), ((0, -pair_count * 4 % 16), (0, 0)))
        reduced, rows, losses = reduce_gradients(
            grad_kv, spaced, jnp.full((1, HEAD_WIDTH), loss_here), pb_count, neg_count
        )
        rows = rows.reshape(-1, spaced.shape[0], spaced.shape[1])[:, : pair_count * 4]
        rows = rows.reshape(pb_count * neg_count * pair_count, -1)
        loss_value = jnp.sum(losses[:, 0, 0])
    else:
        reduced = lax.psum_scatter(grad_kv, both, scatter_dimension=0, tiled=True)
        reduced = reduced.astype(jnp.float32)
        rows = lax.all_gather(last_rows, both, axis=0, tiled=True)
        loss_value = lax.psum(loss_here, "pb")
    index = row * lax.axis_size("neg") + lax.axis_index("neg")
    share = query_weight.shape[0]
    model_width = share * lax.axis_size("pb") * lax.axis_size("neg")
    out_share = out_weight.shape[1]
    normed_cols = lax.dynamic_slice_in_dim(rows, index * share, share, axis=1)
    resid_cols = lax.dynamic_slice_in_dim(rows, model_width + index * out_share, out_share, axis=1)
    rest = 2 * model_width
    all_q = rows[:, rest : rest + width]
    all_context = rows[:, rest + width :]
    grad_query = jnp.dot(normed_cols.T, all_q, preferred_element_type=jnp.float32)
    grad_out = jnp.dot(all_context.T, resid_cols, preferred_element_type=jnp.float32)
    return (
        scores_here[None],
        loss_value,
        grad_input[None],
        grad_query,
        reduced[:, :kv_width],
        reduced[:, kv_width:],
        grad_out,
    )


def solution(mesh):
    placed = (
        P("pb", "neg", None, None),
        P("pb", "neg"),
        P("pb", "neg"),
        P(),
        P(),
        P(),
        P(("pb", "neg"), None),
        P(("pb", "neg"), None),
        P(("pb", "neg"), None),
        P(None, ("pb", "neg")),
    )
    return jax.shard_map(
        shards,
        mesh=mesh,
        in_specs=placed,
        out_specs=(
            P("pb", "neg"),
            P(),
            P("pb", "neg", None, None),
            P(("pb", "neg"), None),
            P(("pb", "neg"), None),
            P(("pb", "neg"), None),
            P(None, ("pb", "neg")),
        ),
        check_vma=False,
    )
```
